128 devices in a mesh: rep: 2 (over core), dp: 64 (over x, y, z).
Axes of the slice: x: 4, y: 4, z: 4, core: 2. Of those that a mesh axis runs over, the one named last changes fastest.
Arguments:
- x: bfloat16 [128, 2048, 1280], P(('rep', 'dp')), parts along dimension 0
- dy: bfloat16 [128, 2048, 1280], P(('rep', 'dp')), parts along dimension 0
- w_gate: bfloat16 [2, 1280, 3584], replicated
- w_up: bfloat16 [2, 1280, 3584], replicated
- w_down: bfloat16 [2, 3584, 1280], replicated
- m_w_gate: float32 [2, 1280, 3584], replicated
- m_w_up: float32 [2, 1280, 3584], replicated
- m_w_down: float32 [2, 3584, 1280], replicated
- v_w_gate: float32 [2, 1280, 3584], replicated
- v_w_up: float32 [2, 1280, 3584], replicated
- v_w_down: float32 [2, 3584, 1280], replicated
Outputs:
- output 1: bfloat16 [4, 1280, 3584], P('rep'), parts along dimension 0
- output 2: bfloat16 [4, 1280, 3584], P('rep'), parts along dimension 0
- output 3: bfloat16 [4, 3584, 1280], P('rep'), parts along dimension 0
- output 4: float32 [4, 1280, 3584], P('rep'), parts along dimension 0
- output 5: float32 [4, 1280, 3584], P('rep'), parts along dimension 0
- output 6: float32 [4, 3584, 1280], P('rep'), parts along dimension 0
- output 7: float32 [4, 1280, 3584], P('rep'), parts along dimension 0
- output 8: float32 [4, 1280, 3584], P('rep'), parts along dimension 0
- output 9: float32 [4, 3584, 1280], P('rep'), parts along dimension 0
There are 2 independent parts. The reference program is written for one: setup_inputs(seed, part) draws one part's arguments, and reference() takes and returns one part's arrays. A program takes and returns all parts, laid end to end along the dimension named above; an argument that names none is the same for every part.
All inputs are finite; a program needn't handle non-finite values.
Results may differ from the reference program's by a relative error of at most 0.022.
Values are sent between devices in bfloat16 or wider.
A program may use at most 1.5 GiB of HBM per device.

```python
import jax
import jax.numpy as jnp
from jax import lax

SEQUENCES = 64
TOKENS = 2048
D = 1280
FF = 3584
LAYERS = 2
NAMES = ("w_gate", "w_up", "w_down")
SHAPES = {"w_gate": (LAYERS, D, FF), "w_up": (LAYERS, D, FF), "w_down": (LAYERS, FF, D)}


def bump(key, n, height):
    away = (jnp.arange(n, dtype=jnp.int32) - jax.random.randint(key, (), 0, n, jnp.int32)) % n
    return jnp.where(away < n // 8, height, 1.0)


def together(key, own, strength):
    shared = jax.random.normal(key, own.shape[1:], jnp.float32)
    return (own + strength * shared) * lax.rsqrt(1 + strength * strength)


def setup_inputs(seed: int = 0, part: int = 0) -> dict:
    kx, kdy, ka, kb, kz, kf, kh, kl, *keys = jax.random.split(jax.random.key(seed), 8 + 3 * len(NAMES))
    kx, kdy, ka, kb = (jax.random.fold_in(k, part) for k in (kx, kdy, ka, kb))
    kw, km, kv = (keys[i::3] for i in range(3))
    shape = (SEQUENCES, TOKENS, D)
    much_x, much_dy = jax.random.uniform(kz, (2,), jnp.float32, 0.0, 1.0)
    loud = 2.0 ** jax.random.uniform(jax.random.fold_in(kz, 1), (), jnp.float32, -1.0, 2.0)
    layers = 2.0 ** jax.random.uniform(kl, (LAYERS, 1, 1), jnp.float32, -1.0, 1.0)
    x = together(ka, jax.random.normal(kx, shape, jnp.float32), much_x) * bump(kf, D, 4.0)
    dy = together(kb, jax.random.normal(kdy, shape, jnp.float32), much_dy)
    drawn = {"x": x.astype(jnp.bfloat16), "dy": (loud * dy * (SEQUENCES * TOKENS) ** -0.5).astype(jnp.bfloat16)}
    for key, name in zip(kw, NAMES, strict=True):
        w = jax.random.normal(key, SHAPES[name], jnp.float32) * SHAPES[name][1] ** -0.5
        drawn[name] = (w * {"w_gate": 1.0, "w_up": bump(kh, FF, 4.0), "w_down": layers}[name]).astype(jnp.bfloat16)
    for key, name in zip(km, NAMES, strict=True):
        drawn[f"m_{name}"] = 0.1 * jax.random.normal(key, SHAPES[name], jnp.float32)
    for key, name in zip(kv, NAMES, strict=True):
        drawn[f"v_{name}"] = loud * loud * jax.random.uniform(key, SHAPES[name], jnp.float32, 0.05, 0.15)
    return drawn


def matmul(a, w):
    return jnp.dot(a, w, preferred_element_type=jnp.float32).astype(jnp.bfloat16)


def normed(h):
    wide = h.astype(jnp.float32)
    scale = lax.rsqrt(jnp.mean(wide**2, -1, keepdims=True) + 1e-6)
    return (wide * scale).astype(jnp.bfloat16)


def layer(h, w):
    a = normed(h)
    gate = jnp.dot(a, w["w_gate"], preferred_element_type=jnp.float32)
    up = jnp.dot(a, w["w_up"], preferred_element_type=jnp.float32)
    return h + matmul((jax.nn.silu(gate) * up).astype(jnp.bfloat16), w["w_down"])


def adamw(w, m, v, g):
    m = 0.9 * m + 0.1 * g
    v = 0.95 * v + 0.05 * g * g
    step = m * lax.rsqrt(v + 1e-8) + 0.1 * w
    return (w - 0.02 * step).astype(jnp.bfloat16), m, v


def stack(weights, h):
    return lax.scan(lambda h, w: (layer(h, w), None), h, weights)[0]


def reference(x, dy, w_gate, w_up, w_down, m_w_gate, m_w_up, m_w_down, v_w_gate, v_w_up, v_w_down):
    weights = dict(zip(NAMES, (w_gate, w_up, w_down), strict=True))

    def take(so_far, sequence):
        h, by_y = sequence
        _, back = jax.vjp(lambda w: stack(w, h), weights)
        return jax.tree.map(lambda total, term: total + term.astype(jnp.float32), so_far, back(by_y)[0]), None

    none_yet = {name: jnp.zeros(w.shape, jnp.float32) for name, w in weights.items()}
    by_weights, _ = lax.scan(take, none_yet, (x, dy))
    gradients = [by_weights[name].astype(jnp.bfloat16).astype(jnp.float32) for name in NAMES]
    new = [
        adamw(w.astype(jnp.float32), m, v, g)
        for w, m, v, g in zip((w_gate, w_up, w_down), (m_w_gate, m_w_up, m_w_down), (v_w_gate, v_w_up, v_w_down), gradients, strict=True)
    ]
    return tuple(one[which] for which in range(3) for one in new)
```

```python
import functools

import jax
import jax.numpy as jnp
from jax import lax
from jax.experimental import pallas as pl
from jax.experimental.pallas import tpu as pltpu
from jax.sharding import PartitionSpec as P

F32, BF16 = jnp.float32, jnp.bfloat16
LANES, TILE, WIDE = 128, 16, 256
C = 512
ROWS = 512
SHARE = 80
VMEM = 67_000_000
AB, ABT, ATB = ((1,), (0,)), ((1,), (1,)), ((0,), (0,))
ANY = pl.BlockSpec(memory_space=pl.ANY)
ONCE = pl.Buffered(buffer_count=1)
TOP, BOTTOM = 1, 0

SIDE = 4
DEVICES = SIDE**3
STRIDES = (SIDE * SIDE, SIDE, 1)
ORDERS = ((0, 1, 2), (1, 2, 0), (2, 0, 1))
MATRICES = range(3)
TO = (1, -1)
LOW, HIGH, EVERY = pl.ds(0, 2), pl.ds(2, 2), slice(None)
HALVES = (LOW, HIGH)


def dot(a, b, dims=AB):
    return lax.dot_general(a, b, (dims, ((), ())), preferred_element_type=F32)


def row_scale(wide):
    return lax.rsqrt(jnp.mean(wide * wide, -1, keepdims=True) + 1e-6)


def normed(h):
    wide = h.astype(F32)
    return (wide * row_scale(wide)).astype(BF16)


def span(i, size):
    return slice(i * size, i * size + size)


def rows_of(i, size):
    return pl.ds(i * size, size)


def vmem(*shape, dtype=BF16):
    return pltpu.VMEM(shape, dtype)


def place_of(me):
    return [me // stride % SIDE for stride in STRIDES]


def near(at, d, by):
    return sum(((a + by) % SIDE if i == d else a) * stride for i, (a, stride) in enumerate(zip(at, STRIDES, strict=True)))


def greet():
    at = place_of(lax.axis_index("dp"))
    for d in range(len(STRIDES)):
        for by in TO:
            pl.semaphore_signal(pltpu.get_barrier_semaphore(), device_id={"dp": near(at, d, by)}, device_id_type=pl.DeviceIdType.MESH)


def meet():
    pl.semaphore_wait(pltpu.get_barrier_semaphore(), len(STRIDES) * len(TO))


def remote(at, sems, index, src, dst, d, by):
    send, recv = sems
    return pltpu.make_async_remote_copy(
        src_ref=src, dst_ref=dst, send_sem=send.at[index], recv_sem=recv.at[index], device_id={"dp": near(at, d, by)}, device_id_type=pl.DeviceIdType.MESH
    )


SEMS = (3, 6, 2)


class Scatter:
    wires = (2.4, 5.0, 0.8, 1.6, 0.3, 0.5)

    def __init__(self, rows, start=0):
        self.rows, self.start = rows, start
        self.cut = -(-rows // (TILE + TILE)) * TILE
        block, line, one = (SIDE, SIDE, rows, LANES), (SIDE, rows, LANES), (rows, LANES)
        shapes = (block,) * 5 + (line,) * 3 + (one,) * 4
        self.n = len(shapes)
        dma = pltpu.SemaphoreType.DMA
        self.scratch = [vmem(*s) for _ in MATRICES for s in shapes] + [dma(SEMS), dma(SEMS), dma((3, 4))]
        self.out_shape = jax.ShapeDtypeStruct((3, rows, LANES), BF16)

    def inputs(self, grads):
        return [g.reshape(SIDE, SIDE, SIDE, -1, LANES) for g in grads]

    def bind(self, grads, out, scratch):
        rows = self.rows
        bufs = [scratch[span(c, self.n)] for c in MATRICES]
        *sems, local = scratch[len(MATRICES) * self.n :]
        at = place_of(lax.axis_index("dp"))
        cuts = (pl.ds(0, self.cut), pl.ds(self.cut, self.rows - self.cut))

        def spot(c, phase, by):
            return (at[ORDERS[c][phase]] + by) % SIDE

        def part(c, i2, i3):
            return (i3, i2) if c == 1 else (i2, i3)

        def of_grad(c, by, rest=(EVERY, EVERY)):
            index = list(rest)
            index.insert(ORDERS[c][0], spot(c, 0, by))
            return grads[c].at[(*index, pl.ds(self.start, rows))]

        def copies(step):
            phase, second = divmod(step, 2)
            made = []
            for c in MATRICES:
                to_right, to_left, own, from_l, from_r, half2, from_l2, from_r2, half3, from_l3, from_r3, _ = bufs[c]
                mine = spot(c, 1, 0)
                if phase == 0:
                    ends = (from_l, from_r) if second else [own.at[part(c, h, EVERY)] for h in HALVES]
                    starts = (to_right, to_left) if second else [of_grad(c, 2, part(c, h, EVERY)) for h in HALVES]
                elif phase == 1:
                    ends = (from_l2, from_r2) if second else [half2.at[h] for h in HALVES]
                    starts = [own.at[part(c, spot(c, 1, by), EVERY) if second else part(c, spot(c, 1, 2), h)] for by, h in zip(TO, HALVES, strict=True)]
                else:
                    ends = (from_l3, from_r3) if second else [half3.at[h] for h in cuts]
                    starts = [own.at[part(c, mine, spot(c, phase, by)) if second else (*part(c, mine, spot(c, phase, 2)), h)] for by, h in zip(TO, cuts, strict=True)]
                for i, (src, dst, by) in enumerate(zip(starts, ends, TO, strict=True)):
                    made.append(remote(at, sems, (c, step, i), src, dst, ORDERS[c][phase], by))
            return made

        def loads(c):
            return [pltpu.make_async_copy(of_grad(c, by), bufs[c][i], local.at[c, i]) for i, by in enumerate(TO)]

        def own_load(c):
            return pltpu.make_async_copy(of_grad(c, 0), bufs[c][2], local.at[c, 2])

        def store(c):
            return pltpu.make_async_copy(bufs[c][-1], out.at[c], local.at[c, 3])

        def wide(ref, *index):
            return ref[index].astype(F32)

        def total(c, *index):
            if len(index) == 2:
                return sum(wide(ref, *part(c, *index)) for ref in bufs[c][2:5])
            return total(c, spot(c, 1, 0), *index) + wide(bufs[c][6], *index) + wide(bufs[c][7], *index)

        def put(c, value, *index):
            bufs[c][2][part(c, *index)] = value.astype(BF16)

        def start(step):
            for copy in copies(step):
                copy.start()

        def arrived(step):
            for copy in copies(step):
                copy.wait_recv()

        def tick0():
            start(0)
            for c in MATRICES:
                for copy in loads(c):
                    copy.start()

        def tick1():
            for c in MATRICES:
                for copy in loads(c):
                    copy.wait()
            arrived(0)
            for c in MATRICES:

                @pl.loop(0, 2 * SIDE)
                def _(i):
                    i2, i3 = i // SIDE, i % SIDE
                    for to, at_end in zip(bufs[c][:2], (part(c, i2, i3), part(c, i2 + 2, i3)), strict=True):
                        to[at_end] = (wide(to, *at_end) + wide(bufs[c][2], *at_end)).astype(BF16)

            start(1)
            for c in MATRICES:
                own_load(c).start()

        def tick2():
            for c in MATRICES:
                own_load(c).wait()
            arrived(1)
            for c in MATRICES:
                far = spot(c, 1, 2)
                pl.loop(0, SIDE)(lambda i: put(c, total(c, far, i), far, i))
            start(2)

        def tick3():
            arrived(2)
            for c in MATRICES:
                right, left = (spot(c, 1, by) for by in TO)
                half = bufs[c][5]

                @pl.loop(0, 2)
                def _(i):
                    put(c, total(c, right, i) + wide(half, i), right, i)
                    put(c, total(c, left, i), left, i)
                    put(c, total(c, right, i + 2), right, i + 2)
                    put(c, total(c, left, i + 2) + wide(half, i + 2), left, i + 2)

            start(3)

        def tick4():
            arrived(3)
            for c in MATRICES:
                put(c, total(c, spot(c, 2, 2)), spot(c, 1, 0), spot(c, 2, 2))
            start(4)

        def tick5():
            arrived(4)
            for c in MATRICES:
                sums = [total(c, spot(c, 2, by)) for by in TO]
                for i, by in enumerate(TO):
                    for j, cut in enumerate(cuts):
                        value = sums[i][cut.start : cut.start + cut.size]
                        if i == j:
                            value = value + wide(bufs[c][8], cut)
                        bufs[c][2][(*part(c, spot(c, 1, 0), spot(c, 2, by)), cut)] = value.astype(BF16)
            start(5)

        def tick6():
            arrived(5)
            for c in MATRICES:
                *_, left, right, done = bufs[c]
                done[...] = (total(c, spot(c, 2, 0)) + wide(left, ...) + wide(right, ...)).astype(BF16)
                store(c).start()
            for step in range(len(self.wires)):
                for copy in copies(step):
                    copy.wait_send()
            for c in MATRICES:
                store(c).wait()

        return tick0, tick1, tick2, tick3, tick4, tick5, tick6


class Exchange:
    def __init__(self, key=None, *moves):
        self.moves = [move for move, _ in moves]
        self.inputs = [move.inputs(arrays) for move, arrays in moves]
        self.in_arrays = sum(self.inputs, [])
        self.in_specs = [ANY] * len(self.in_arrays)
        self.out_specs = [ANY] * len(moves)
        self.out_shapes = [move.out_shape for move in self.moves]
        self.scratch = sum((move.scratch for move in self.moves), [])
        talks = dict(collective_id=key, has_side_effects=True) if moves else {}
        self.params = pltpu.CompilerParams(vmem_limit_bytes=VMEM, **talks)

    def split(self, refs, n_in, n_out):
        a = n_in + len(self.in_arrays)
        b = a + n_out + len(self.moves)
        end = len(refs) - len(self.scratch)
        own = refs[:n_in] + refs[a : a + n_out] + refs[b:end]
        return own, (list(refs[n_in:a]), list(refs[a + n_out : b]), list(refs[end:]))

    def bind(self, refs):
        ins, outs, scratch = refs
        ticks = []
        for move, arrays, out in zip(self.moves, self.inputs, outs, strict=True):
            ticks.append(move.bind(ins[: len(arrays)], out, scratch[: len(move.scratch)]))
            ins, scratch = ins[len(arrays) :], scratch[len(move.scratch) :]
        return ticks

    def plan(self, steps, lengths):
        ends, now = [], 0.0
        for length in lengths * steps:
            now += length
            ends.append(now)
        plans = []
        for move in self.moves:
            others = sum(other.rows for other in self.moves) - move.rows
            units = (move.rows + 0.6 * others) / SHARE
            now, where = ends[0], [0]
            for wire in move.wires:
                now += 3.5 + wire * units
                where.append(min(sum(end < now for end in ends), len(ends) - 1))
            where[-1] = len(ends) - 1
            plans.append(where)
        return plans

    def sites(self, refs, steps, lengths):
        if not self.moves:
            return lambda piece: None
        step = pl.program_id(0)
        pl.when(step == 0)(greet)
        pairs = [pair for ticks, where in zip(self.bind(refs), self.plan(steps, lengths), strict=True) for pair in zip(where, ticks, strict=True)]

        def site(piece):
            if piece == 0:
                pl.when(step == 0)(meet)
            for place, tick in pairs:
                if place % len(lengths) == piece:
                    pl.when(step == place // len(lengths))(tick)

        return site

    def alone(self):
        def body(*refs):
            _, extra = self.split(refs, 0, 0)
            greet()
            meet()
            for ticks in zip(*self.bind(extra), strict=True):
                for tick in ticks:
                    tick()

        return pl.pallas_call(
            body,
            in_specs=self.in_specs,
            out_specs=self.out_specs,
            out_shape=self.out_shapes,
            scratch_shapes=self.scratch,
            compiler_params=self.params,
            cost_estimate=pl.CostEstimate(flops=60_000_000_000, bytes_accessed=20_000_000, transcendentals=0),
            name="exchange",
        )(*self.in_arrays)


def swiglu_back(gate, up, dhid):
    sig = lax.logistic(gate)
    silu = gate * sig
    d = dhid.astype(BF16).astype(F32)
    hid = (silu * up).astype(BF16)
    dup = (d * silu).astype(BF16)
    dgate = (d * up * (sig + silu * (1.0 - sig))).astype(BF16)
    return hid, dgate, dup


def put_gradients(a, dy, hid, dgate, dup, gg, gu, gd, site, piece):
    D = a.shape[1]
    for k in range(D // WIDE):
        value = dot(hid[...], dy[:, span(k, WIDE)], ATB).astype(BF16)
        for i in range(C // TILE):
            for j in range(WIDE // LANES):
                half, tile = divmod(WIDE // LANES * k + j, SHARE // TILE)
                gd[2 * i + half, rows_of(tile, TILE)] = value[span(i, TILE), span(j, LANES)]
    site(piece)
    for k in range(2):
        part = a[:, span(k, D // 2)]
        for out, by in ((gg, dgate), (gu, dup)):
            value = dot(part, by[...], ATB).astype(BF16)
            for i in range(D // 2 // SHARE):
                for j in range(C // LANES):
                    out[(D // 2 // SHARE * k + i) * SIDE + j] = value[span(i, SHARE), span(j, LANES)]
        site(piece + 1 + k)


def top_unit(a, dy, wg, wu, wd, gg, gu, gd, dgate_o, dup_o, hid, site, ready):
    blocks = a.shape[0] // ROWS
    for i in range(blocks):
        ready(i)
        r = rows_of(i, ROWS)
        gate = dot(a[r, :], wg[0])
        up = dot(a[r, :], wu[0])
        dhid = dot(dy[r, :], wd[0], ABT)
        hid[r, :], dgate_o[r, :], dup_o[r, :] = swiglu_back(gate, up, dhid)
        site(i)
    put_gradients(a, dy, hid, dgate_o, dup_o, gg, gu, gd, site, blocks)


def by_rows(source, target, sem):
    return [pltpu.make_async_copy(source.at[r], target.at[r], sem.at[i]) for i in range(target.shape[0] // ROWS) for r in (rows_of(i, ROWS),)]


UNIT = pl.BlockSpec((DEVICES, SHARE, LANES), lambda j: (0, j, 0))


def unit_shapes(count):
    return [jax.ShapeDtypeStruct((DEVICES, SHARE * count, LANES), BF16)] * len(MATRICES)


def top_body(exchange, count, n_chain, *refs):
    own, extra = exchange.split(refs, 5 + n_chain, 5)
    a, dy, wg, wu, wd = own[:5]
    *outs, hid, a_v, dy_v, sem = own[5 + n_chain :]
    step = pl.program_id(0)
    loads = list(zip(by_rows(a, a_v, sem.at[0]), by_rows(dy, dy_v, sem.at[1]), strict=True))

    @pl.when(step == 0)
    def _():
        for pair in loads:
            for copy in pair:
                copy.start()

    def ready(i):
        if i < 2:

            @pl.when(step == 0)
            def _():
                for pair in loads[i:] if i else loads[:1]:
                    for copy in pair:
                        copy.wait()

    site = exchange.sites(extra, count, (2.6, 2.4, 2.4, 2.4, 2.7, 2.7, 2.7))
    top_unit(a_v, dy_v, wg, wu, wd, *outs, hid, site, ready)


def top(a, dy, wg, wu, wd, first, count, so_far, exchange):
    T, D = a.shape
    FF = wg.shape[-1]
    col = pl.BlockSpec((1, D, C), lambda j: (TOP, 0, first + j))
    act = pl.BlockSpec((T, C), lambda j: (0, first + j))
    W = C * count
    return pl.pallas_call(
        functools.partial(top_body, exchange, count, len(so_far)),
        grid=(count,),
        in_specs=[ANY, ANY, col, col, pl.BlockSpec((1, C, D), lambda j: (TOP, first + j, 0))] + [ANY] * len(so_far) + exchange.in_specs,
        input_output_aliases={5 + i: 3 + i for i in range(len(so_far))},
        out_specs=[UNIT] * 3 + [act, act] + exchange.out_specs,
        out_shape=unit_shapes(count) + [jax.ShapeDtypeStruct((T, FF), BF16)] * 2 + exchange.out_shapes,
        scratch_shapes=[vmem(T, C), vmem(T, D), vmem(T, D), pltpu.SemaphoreType.DMA((2, T // ROWS))] + exchange.scratch,
        compiler_params=exchange.params,
        cost_estimate=pl.CostEstimate(flops=12 * T * D * W, bytes_accessed=20_000_000, transcendentals=T * W),
        name=f"top{first}",
    )(a, dy, wg, wu, wd, *so_far, *exchange.in_arrays)


def bottom_body(exchange, count, *refs):
    own, extra = exchange.split(refs, 5, 3)
    a, dy, gate, up, wd, gg, gu, gd, hid, dgate, dup = own
    site = exchange.sites(extra, count, (5.0, 2.9, 2.9, 2.9))
    for i in range(a.shape[0] // ROWS):
        r = rows_of(i, ROWS)
        dhid = dot(dy[r, :], wd[0], ABT)
        hid[r, :], dgate[r, :], dup[r, :] = swiglu_back(gate[0, r, :], up[0, r, :], dhid)
    site(0)
    put_gradients(a, dy, hid, dgate, dup, gg, gu, gd, site, 1)


def bottom(a, dy, gate, up, wd, first, count, exchange):
    T, D = a.shape
    whole = pl.BlockSpec((T, D), lambda j: (0, 0), pipeline_mode=ONCE)
    act = pl.BlockSpec((1, T, C), lambda j: (first + j, 0, 0))
    W = C * count
    return pl.pallas_call(
        functools.partial(bottom_body, exchange, count),
        grid=(count,),
        in_specs=[whole, whole, act, act, pl.BlockSpec((1, C, D), lambda j: (BOTTOM, first + j, 0))] + exchange.in_specs,
        out_specs=[UNIT] * 3 + exchange.out_specs,
        out_shape=unit_shapes(count) + exchange.out_shapes,
        scratch_shapes=[vmem(T, C)] * 3 + exchange.scratch,
        compiler_params=exchange.params,
        cost_estimate=pl.CostEstimate(flops=8 * T * D * W, bytes_accessed=20_000_000, transcendentals=T * W),
        name=f"bottom{first}",
    )(a, dy, gate, up, wd, *exchange.in_arrays)


def through_body(exchange, steps, *refs):
    own, extra = exchange.split(refs, 6, 1)
    h1, dy, wg, wu, dgate, dup, dh_o, wg_v, wu_v, sem = own
    D = h1.shape[1]
    parts = D // WIDE
    step = pl.program_id(0)
    blocks = [rows_of(k, WIDE) for k in range(parts)]
    loads = [[pltpu.make_async_copy(w.at[TOP, n], v.at[n], sem.at[i, k]) for i, (w, v) in enumerate(((wg, wg_v), (wu, wu_v)))] for k, n in enumerate(blocks)]

    @pl.when(step == 0)
    def _():
        for pair in loads:
            for copy in pair:
                copy.start()

    site = exchange.sites(extra, steps, (2.2,) * (parts - 1) + (3.5,))
    for k, n in enumerate(blocks):
        if k <= 2:

            @pl.when(step == 0)
            def _():
                for pair in loads[k:] if k == 2 else loads[k : k + 1]:
                    for copy in pair:
                        copy.wait()

        dh_o[:, n] = dot(dgate[...], wg_v[n, :], ABT).astype(BF16) + dot(dup[...], wu_v[n, :], ABT).astype(BF16)
        if k < parts - 1:
            site(k)
    by_a = dh_o[...].astype(F32)
    wide = h1[...].astype(F32)
    scale = row_scale(wide)
    by_scale = jnp.sum(by_a * wide, -1, keepdims=True)
    by_mean = by_scale * (-scale * scale * scale / D)
    dh_o[...] = dy[...] + (by_a * scale + wide * by_mean).astype(BF16)
    site(parts - 1)


def through(h1, dy, wg, wu, dgate, dup, exchange):
    T, D = h1.shape
    FF = wg.shape[-1]
    act = pl.BlockSpec((ROWS, FF), lambda j: (j, 0))
    state = pl.BlockSpec((ROWS, D), lambda j: (j, 0))
    return pl.pallas_call(
        functools.partial(through_body, exchange, T // ROWS),
        grid=(T // ROWS,),
        in_specs=[state, state, ANY, ANY, act, act] + exchange.in_specs,
        out_specs=[state] + exchange.out_specs,
        out_shape=[jax.ShapeDtypeStruct((T, D), BF16)] + exchange.out_shapes,
        scratch_shapes=[vmem(D, FF)] * 2 + [pltpu.SemaphoreType.DMA((2, D // WIDE))] + exchange.scratch,
        compiler_params=exchange.params,
        cost_estimate=pl.CostEstimate(flops=4 * T * D * FF, bytes_accessed=60_000_000, transcendentals=T),
        name="through",
    )(h1, dy, wg, wu, dgate, dup, *exchange.in_arrays)


def forward_body(steps, x, dy, wg, wu, wd, gate_o, up_o, a0_o, h1_o, a1_o, gg, gu, gd, dgate_o, dup_o, h, a, acc, hid, sem):
    j = pl.program_id(0)
    T, D = h.shape
    blocks = T // ROWS
    load, load_dy, save_h1, save_a1 = (
        by_rows(*pair, sem.at[i]) if i < 2 else [pltpu.make_async_copy(pair[0].at[r], pair[1].at[r], sem.at[i, k]) for k in range(blocks) for r in (rows_of(k, ROWS),)]
        for i, pair in enumerate(((x, h), (dy, h), (h, h1_o), (a, a1_o)))
    )
    save_a0 = pltpu.make_async_copy(a, a0_o, sem.at[4, 0])

    @pl.when(j == 0)
    def _():
        for copy in load:
            copy.start()
        for i in range(blocks):
            load[i].wait()

            @pl.loop(i * ROWS // LANES, (i + 1) * ROWS // LANES)
            def _(k):
                r = rows_of(k, LANES)
                a[r, :] = normed(h[r, :])
                acc[r, :] = jnp.zeros((LANES, D), F32)

        save_a0.start()

    @pl.when(j < steps)
    def _():
        half = T // 2

        @pl.loop(0, 2)
        def _(i):
            r = rows_of(i, half)
            gate = dot(a[r, :], wg[0])
            up = dot(a[r, :], wu[0])
            gate_o[0, r, :] = gate
            up_o[0, r, :] = up
            hid[r, :] = (gate * lax.logistic(gate) * up).astype(BF16)

        @pl.loop(0, 2)
        def _(i):
            r = rows_of(i, half)
            for k in range(D // WIDE):
                n = span(k, WIDE)
                acc[r, n] += dot(hid[r, :], wd[0, :, n])

    @pl.when(j == steps - 1)
    def _():
        save_a0.wait()
        for i in range(blocks):

            @pl.loop(i * ROWS // LANES, (i + 1) * ROWS // LANES)
            def _(k):
                r = rows_of(k, LANES)
                new = h[r, :] + acc[r, :].astype(BF16)
                h[r, :] = new
                a[r, :] = normed(new)

            save_h1[i].start()
            save_a1[i].start()

    @pl.when(j == steps)
    def _():
        for save, load in zip(save_h1, load_dy, strict=True):
            save.wait()
            load.start()
        top_unit(a, h, wg, wu, wd, gg, gu, gd, dgate_o, dup_o, hid, lambda piece: None, lambda i: load_dy[i].wait())
        for copy in save_a1:
            copy.wait()


def forward(x, dy, wg, wu, wd):
    T, D = x.shape
    FF = wg.shape[-1]
    n = FF // C
    col = pl.BlockSpec((1, D, C), lambda j: (j // n, 0, j % n))
    act = pl.BlockSpec((1, T, C), lambda j: (jnp.minimum(j, n - 1), 0, 0))
    unit = pl.BlockSpec((DEVICES, SHARE, LANES), lambda j: (0, 0, 0), pipeline_mode=ONCE)
    back = pl.BlockSpec((T, C), lambda j: (0, 0), pipeline_mode=ONCE)
    return pl.pallas_call(
        functools.partial(forward_body, n),
        grid=(n + 1,),
        in_specs=[ANY, ANY, col, col, pl.BlockSpec((1, C, D), lambda j: (j // n, j % n, 0))],
        out_specs=[act, act, ANY, ANY, ANY, unit, unit, unit, back, back],
        out_shape=[jax.ShapeDtypeStruct((n, T, C), F32)] * 2
        + [jax.ShapeDtypeStruct((T, D), BF16)] * 3
        + unit_shapes(1)
        + [jax.ShapeDtypeStruct((T, FF), BF16)] * 2,
        scratch_shapes=[vmem(T, D), vmem(T, D), vmem(T, D, dtype=F32), vmem(T, C), pltpu.SemaphoreType.DMA((5, T // ROWS))],
        compiler_params=pltpu.CompilerParams(vmem_limit_bytes=VMEM),
        cost_estimate=pl.CostEstimate(flops=6 * T * D * FF, bytes_accessed=100_000_000, transcendentals=T * FF),
        name="forward",
    )(x, dy, wg, wu, wd)


def new_values(w, m, v, g):
    m = 0.9 * m + 0.1 * g
    v = 0.95 * v + 0.05 * g * g
    step = m * lax.rsqrt(v + 1e-8) + 0.1 * w
    return (w - 0.02 * step).astype(BF16), m, v


def adamw_body(*refs):
    g, w, m, v = (refs[span(i, 3)] for i in range(4))
    new = refs[-9:]
    for which in MATRICES:

        def take(rows, cols, grad):
            at = (0, rows, cols)
            done = new_values(w[which][at].astype(F32), m[which][at], v[which][at], grad.astype(F32))
            for out, value in zip(new[which::3], done, strict=True):
                out[at] = value

        _, rows, cols = w[which].shape
        if which < 2:
            for i in range(rows // SHARE):
                for j in range(SIDE):
                    take(rows_of(i, SHARE), rows_of(j, LANES), g[which][i * SIDE + j, 0])
        else:
            for i in range(rows // TILE):
                for j in range(cols // LANES):
                    half, tile = divmod(j, SHARE // TILE)
                    take(rows_of(i, TILE), rows_of(j, LANES), g[which][2 * i + half, 0, rows_of(tile, TILE), :])


def adamw(summed, arrays, layer, first, count, so_far):
    D = arrays[0].shape[1]
    summed = summed.reshape(DEVICES, 3, SHARE * count, LANES)

    def grad(which):
        return pl.BlockSpec((DEVICES // SIDE, 1, SHARE, LANES), lambda i: (i % SIDE, which, i // SIDE, 0))

    wide = pl.BlockSpec((1, D // SIDE, C), lambda i: (layer, i % SIDE, first + i // SIDE))
    tall = pl.BlockSpec((1, C // SIDE, D), lambda i: (layer, first * SIDE + i, 0))
    nine = [wide, wide, tall] * 3
    return pl.pallas_call(
        adamw_body,
        grid=(count * SIDE,),
        in_specs=[grad(which) for which in MATRICES] + nine + [ANY] * len(so_far),
        out_specs=nine,
        out_shape=[jax.ShapeDtypeStruct(a.shape, a.dtype) for a in arrays],
        input_output_aliases={12 + i: i for i in range(len(so_far))},
        compiler_params=pltpu.CompilerParams(vmem_limit_bytes=VMEM),
        cost_estimate=pl.CostEstimate(flops=1_000_000_000 * count, bytes_accessed=66 * D * C * count, transcendentals=3 * D * C * count),
        name=f"adamw{layer}_{first}",
    )(summed, summed, summed, *arrays, *so_far)


def solution(mesh):
    def step(x, dy, *arrays):
        x, dy = x[0], dy[0]
        weights = arrays[:3]
        *gates, wd = weights
        one, three, four = (SHARE * count for count in (1, 3, 4))
        gate0, up0, a0, h1, a1, *out = forward(x, dy, *weights)
        g0, back = out[:3], out[3:]
        *out, s0 = top(a1, dy, *weights, 1, 3, back, Exchange(1, (Scatter(one), g0)))
        g1, back = out[:3], out[3:]
        *out, s1 = top(a1, dy, *weights, 4, 3, back, Exchange(2, (Scatter(three), g1)))
        g2, back = out[:3], out[3:]
        dh1, s2 = through(h1, dy, *gates, *back, Exchange(3, (Scatter(three), g2)))
        g3 = bottom(a0, dh1, gate0, up0, wd, 0, 3, Exchange())
        *g4, s3 = bottom(a0, dh1, gate0, up0, wd, 3, 4, Exchange(4, (Scatter(three), g3)))
        (s4,) = Exchange(5, (Scatter(four), g4)).alone()
        new = ()
        for shard, layer, first, count in ((jnp.concatenate([s0, s1, s2], 1), TOP, 0, 7), (s3, BOTTOM, 0, 3), (s4, BOTTOM, 3, 4)):
            new = adamw(lax.all_gather(shard, "dp", axis=0, tiled=False), arrays, layer, first, count, new)
        return tuple(new)

    whole = P(None, None, None)
    return jax.shard_map(
        step, mesh=mesh, in_specs=(P(("rep", "dp"), None, None),) * 2 + (whole,) * 9, out_specs=(P("rep", None, None),) * 9, check_vma=False
    )
```

```python
import functools

import jax
import jax.numpy as jnp
from jax import lax
from jax.experimental import pallas as pl
from jax.experimental.pallas import tpu as pltpu
from jax.sharding import PartitionSpec as P

F32, BF16 = jnp.float32, jnp.bfloat16
LANES, TILE, WIDE = 128, 16, 256
C = 512
ROWS = 512
SHARE = 80
VMEM = 67_000_000
AB, ABT, ATB = ((1,), (0,)), ((1,), (1,)), ((0,), (0,))
ANY = pl.BlockSpec(memory_space=pl.ANY)
ONCE = pl.Buffered(buffer_count=1)
TOP, BOTTOM = 1, 0
STEPS = 2

SIDE = 4
DEVICES = SIDE**3
STRIDES = (SIDE * SIDE, SIDE, 1)
ORDERS = ((0, 1, 2), (1, 2, 0), (2, 0, 1))
MATRICES = range(3)
TO = (1, -1)
LOW, HIGH, EVERY = pl.ds(0, 2), pl.ds(2, 2), slice(None)
HALVES = (LOW, HIGH)


def dot(a, b, dims=AB):
    return lax.dot_general(a, b, (dims, ((), ())), preferred_element_type=F32)


def row_scale(wide):
    return lax.rsqrt(jnp.mean(wide * wide, -1, keepdims=True) + 1e-6)


def normed(h):
    wide = h.astype(F32)
    return (wide * row_scale(wide)).astype(BF16)


def span(i, size):
    return slice(i * size, i * size + size)


def rows_of(i, size):
    return pl.ds(i * size, size)


def vmem(*shape, dtype=BF16):
    return pltpu.VMEM(shape, dtype)


def place_of(me):
    return [me // stride % SIDE for stride in STRIDES]


def near(at, d, by):
    return sum(((a + by) % SIDE if i == d else a) * stride for i, (a, stride) in enumerate(zip(at, STRIDES, strict=True)))


def greet():
    at = place_of(lax.axis_index("dp"))
    for d in range(len(STRIDES)):
        for by in TO:
            pl.semaphore_signal(pltpu.get_barrier_semaphore(), device_id={"dp": near(at, d, by)}, device_id_type=pl.DeviceIdType.MESH)


def meet():
    pl.semaphore_wait(pltpu.get_barrier_semaphore(), len(STRIDES) * len(TO))


def remote(at, sems, index, src, dst, d, by):
    send, recv = sems
    return pltpu.make_async_remote_copy(
        src_ref=src, dst_ref=dst, send_sem=send.at[index], recv_sem=recv.at[index], device_id={"dp": near(at, d, by)}, device_id_type=pl.DeviceIdType.MESH
    )


SEMS = (3, 6, 2)


class Scatter:
    wires = (2.2, 4.6, 0.7, 1.5, 0.3, 0.5)

    def __init__(self, rows, start=0):
        self.rows, self.start = rows, start
        self.cut = -(-rows // (TILE + TILE)) * TILE
        block, line, one = (SIDE, SIDE, rows, LANES), (SIDE, rows, LANES), (rows, LANES)
        shapes = (block,) * 5 + (line,) * 3 + (one,) * 4
        self.n = len(shapes)
        dma = pltpu.SemaphoreType.DMA
        self.scratch = [vmem(*s) for _ in MATRICES for s in shapes] + [dma(SEMS), dma(SEMS), dma((3, 4))]
        self.out_shape = jax.ShapeDtypeStruct((3, rows, LANES), BF16)

    def inputs(self, grads):
        return [g.reshape(SIDE, SIDE, SIDE, -1, LANES) for g in grads]

    def bind(self, grads, out, scratch):
        rows = self.rows
        bufs = [scratch[span(c, self.n)] for c in MATRICES]
        *sems, local = scratch[len(MATRICES) * self.n :]
        at = place_of(lax.axis_index("dp"))
        cuts = (pl.ds(0, self.cut), pl.ds(self.cut, self.rows - self.cut))

        def spot(c, phase, by):
            return (at[ORDERS[c][phase]] + by) % SIDE

        def part(c, i2, i3):
            return (i3, i2) if c == 1 else (i2, i3)

        def of_grad(c, by, rest=(EVERY, EVERY)):
            index = list(rest)
            index.insert(ORDERS[c][0], spot(c, 0, by))
            return grads[c].at[(*index, pl.ds(self.start, rows))]

        def copies(step):
            phase, second = divmod(step, 2)
            made = []
            for c in MATRICES:
                to_right, to_left, own, from_l, from_r, half2, from_l2, from_r2, half3, from_l3, from_r3, _ = bufs[c]
                mine = spot(c, 1, 0)
                if phase == 0:
                    ends = (from_l, from_r) if second else [own.at[part(c, h, EVERY)] for h in HALVES]
                    starts = (to_right, to_left) if second else [of_grad(c, 2, part(c, h, EVERY)) for h in HALVES]
                elif phase == 1:
                    ends = (from_l2, from_r2) if second else [half2.at[h] for h in HALVES]
                    starts = [own.at[part(c, spot(c, 1, by), EVERY) if second else part(c, spot(c, 1, 2), h)] for by, h in zip(TO, HALVES, strict=True)]
                else:
                    ends = (from_l3, from_r3) if second else [half3.at[h] for h in cuts]
                    starts = [own.at[part(c, mine, spot(c, phase, by)) if second else (*part(c, mine, spot(c, phase, 2)), h)] for by, h in zip(TO, cuts, strict=True)]
                for i, (src, dst, by) in enumerate(zip(starts, ends, TO, strict=True)):
                    made.append(remote(at, sems, (c, step, i), src, dst, ORDERS[c][phase], by))
            return made

        def loads(c):
            return [pltpu.make_async_copy(of_grad(c, by), bufs[c][i], local.at[c, i]) for i, by in enumerate(TO)]

        def own_load(c):
            return pltpu.make_async_copy(of_grad(c, 0), bufs[c][2], local.at[c, 2])

        def store(c):
            return pltpu.make_async_copy(bufs[c][-1], out.at[c], local.at[c, 3])

        def wide(ref, *index):
            return ref[index].astype(F32)

        def total(c, *index):
            if len(index) == 2:
                return sum(wide(ref, *part(c, *index)) for ref in bufs[c][2:5])
            return total(c, spot(c, 1, 0), *index) + wide(bufs[c][6], *index) + wide(bufs[c][7], *index)

        def put(c, value, *index):
            bufs[c][2][part(c, *index)] = value.astype(BF16)

        def start(step):
            for copy in copies(step):
                copy.start()

        def arrived(step):
            for copy in copies(step):
                copy.wait_recv()

        def tick0():
            start(0)
            for c in MATRICES:
                for copy in loads(c):
                    copy.start()

        def tick1():
            for c in MATRICES:
                for copy in loads(c):
                    copy.wait()
            arrived(0)
            for c in MATRICES:

                @pl.loop(0, 2 * SIDE)
                def _(i):
                    i2, i3 = i // SIDE, i % SIDE
                    for to, at_end in zip(bufs[c][:2], (part(c, i2, i3), part(c, i2 + 2, i3)), strict=True):
                        to[at_end] = (wide(to, *at_end) + wide(bufs[c][2], *at_end)).astype(BF16)

            start(1)
            for c in MATRICES:
                own_load(c).start()

        def tick2():
            for c in MATRICES:
                own_load(c).wait()
            arrived(1)
            for c in MATRICES:
                far = spot(c, 1, 2)
                pl.loop(0, SIDE)(lambda i: put(c, total(c, far, i), far, i))
            start(2)

        def tick3():
            arrived(2)
            for c in MATRICES:
                right, left = (spot(c, 1, by) for by in TO)
                half = bufs[c][5]

                @pl.loop(0, 2)
                def _(i):
                    put(c, total(c, right, i) + wide(half, i), right, i)
                    put(c, total(c, left, i), left, i)
                    put(c, total(c, right, i + 2), right, i + 2)
                    put(c, total(c, left, i + 2) + wide(half, i + 2), left, i + 2)

            start(3)

        def tick4():
            arrived(3)
            for c in MATRICES:
                put(c, total(c, spot(c, 2, 2)), spot(c, 1, 0), spot(c, 2, 2))
            start(4)

        def tick5():
            arrived(4)
            for c in MATRICES:
                sums = [total(c, spot(c, 2, by)) for by in TO]
                for i, by in enumerate(TO):
                    for j, cut in enumerate(cuts):
                        value = sums[i][cut.start : cut.start + cut.size]
                        if i == j:
                            value = value + wide(bufs[c][8], cut)
                        bufs[c][2][(*part(c, spot(c, 1, 0), spot(c, 2, by)), cut)] = value.astype(BF16)
            start(5)

        def tick6():
            arrived(5)
            for c in MATRICES:
                *_, left, right, done = bufs[c]
                done[...] = (total(c, spot(c, 2, 0)) + wide(left, ...) + wide(right, ...)).astype(BF16)
                store(c).start()
            for step in range(len(self.wires)):
                for copy in copies(step):
                    copy.wait_send()
            for c in MATRICES:
                store(c).wait()

        return tick0, tick1, tick2, tick3, tick4, tick5, tick6


class Exchange:
    def __init__(self, key=None, *moves):
        self.moves = [move for move, _ in moves]
        self.inputs = [move.inputs(arrays) for move, arrays in moves]
        self.in_arrays = sum(self.inputs, [])
        self.in_specs = [ANY] * len(self.in_arrays)
        self.out_specs = [ANY] * len(moves)
        self.out_shapes = [move.out_shape for move in self.moves]
        self.scratch = sum((move.scratch for move in self.moves), [])
        talks = dict(collective_id=key, has_side_effects=True) if moves else {}
        self.params = pltpu.CompilerParams(vmem_limit_bytes=VMEM, **talks)

    def split(self, refs, n_in, n_out):
        a = n_in + len(self.in_arrays)
        b = a + n_out + len(self.moves)
        end = len(refs) - len(self.scratch)
        own = refs[:n_in] + refs[a : a + n_out] + refs[b:end]
        return own, (list(refs[n_in:a]), list(refs[a + n_out : b]), list(refs[end:]))

    def bind(self, refs):
        ins, outs, scratch = refs
        ticks = []
        for move, arrays, out in zip(self.moves, self.inputs, outs, strict=True):
            ticks.append(move.bind(ins[: len(arrays)], out, scratch[: len(move.scratch)]))
            ins, scratch = ins[len(arrays) :], scratch[len(move.scratch) :]
        return ticks

    def plan(self, steps, lengths):
        ends, now = [], 0.0
        for length in lengths * steps:
            now += length
            ends.append(now)
        plans = []
        for move in self.moves:
            waits = [3.0 + wire * move.rows / SHARE for wire in move.wires]
            stretch = min(max((ends[-1] - ends[0]) / sum(waits), 1.0), 1.6)
            now, where = ends[0], [0]
            for wait in waits:
                now += wait * stretch
                where.append(min(sum(end < now for end in ends), len(ends) - 1))
            where[-1] = len(ends) - 1
            plans.append(where)
        return plans

    def sites(self, refs, steps, lengths):
        if not self.moves:
            return lambda piece: None
        step = pl.program_id(0)
        pl.when(step == 0)(greet)
        pairs = [pair for ticks, where in zip(self.bind(refs), self.plan(steps, lengths), strict=True) for pair in zip(where, ticks, strict=True)]

        def site(piece):
            if piece == 0:
                pl.when(step == 0)(meet)
            for place, tick in pairs:
                if place % len(lengths) == piece:
                    pl.when(step == place // len(lengths))(tick)

        return site

    def alone(self):
        def body(*refs):
            _, extra = self.split(refs, 0, 0)
            greet()
            meet()
            for ticks in zip(*self.bind(extra), strict=True):
                for tick in ticks:
                    tick()

        return pl.pallas_call(
            body,
            in_specs=self.in_specs,
            out_specs=self.out_specs,
            out_shape=self.out_shapes,
            scratch_shapes=self.scratch,
            compiler_params=self.params,
            cost_estimate=pl.CostEstimate(flops=60_000_000_000, bytes_accessed=20_000_000, transcendentals=0),
            name="exchange",
        )(*self.in_arrays)


def swiglu_back(gate, up, dhid):
    sig = lax.logistic(gate)
    silu = gate * sig
    d = dhid.astype(BF16).astype(F32)
    hid = (silu * up).astype(BF16)
    dup = (d * silu).astype(BF16)
    dgate = (d * up * (sig + silu * (1.0 - sig))).astype(BF16)
    return hid, dgate, dup


def put_gradients(a, dy, hid, dgate, dup, gg, gu, gd, site, piece):
    D = a.shape[1]
    for k in range(D // WIDE):
        value = dot(hid[...], dy[:, span(k, WIDE)], ATB).astype(BF16)
        for i in range(C // TILE):
            for j in range(WIDE // LANES):
                half, tile = divmod(WIDE // LANES * k + j, SHARE // TILE)
                gd[2 * i + half, rows_of(tile, TILE)] = value[span(i, TILE), span(j, LANES)]
    site(piece)
    for k in range(2):
        part = a[:, span(k, D // 2)]
        for out, by in ((gg, dgate), (gu, dup)):
            value = dot(part, by[...], ATB).astype(BF16)
            for i in range(D // 2 // SHARE):
                for j in range(C // LANES):
                    out[(D // 2 // SHARE * k + i) * SIDE + j] = value[span(i, SHARE), span(j, LANES)]
        site(piece + 1 + k)


def top_unit(a, dy, wg, wu, wd, gg, gu, gd, dgate_o, dup_o, hid, site, ready):
    blocks = a.shape[0] // ROWS
    for i in range(blocks):
        ready(i)
        r = rows_of(i, ROWS)
        gate = dot(a[r, :], wg[0])
        up = dot(a[r, :], wu[0])
        dhid = dot(dy[r, :], wd[0], ABT)
        hid[r, :], dgate_o[r, :], dup_o[r, :] = swiglu_back(gate, up, dhid)
        site(i)
    put_gradients(a, dy, hid, dgate_o, dup_o, gg, gu, gd, site, blocks)


def by_rows(source, target, sem):
    return [pltpu.make_async_copy(source.at[r], target.at[r], sem.at[i]) for i in range(target.shape[0] // ROWS) for r in (rows_of(i, ROWS),)]


UNIT = pl.BlockSpec((DEVICES, SHARE, LANES), lambda j: (0, j, 0))


def unit_shapes(count):
    return [jax.ShapeDtypeStruct((DEVICES, SHARE * count, LANES), BF16)] * len(MATRICES)


def top_body(exchange, count, n_chain, *refs):
    own, extra = exchange.split(refs, 5 + n_chain, 5)
    a, dy, wg, wu, wd = own[:5]
    *outs, hid, a_v, dy_v, sem = own[5 + n_chain :]
    step = pl.program_id(0)
    loads = list(zip(by_rows(a, a_v, sem.at[0]), by_rows(dy, dy_v, sem.at[1]), strict=True))

    @pl.when(step == 0)
    def _():
        for pair in loads:
            for copy in pair:
                copy.start()

    def ready(i):
        if i < 2:

            @pl.when(step == 0)
            def _():
                for pair in loads[i:] if i else loads[:1]:
                    for copy in pair:
                        copy.wait()

    site = exchange.sites(extra, count, (2.6, 2.4, 2.4, 2.4, 2.7, 2.7, 2.7))
    top_unit(a_v, dy_v, wg, wu, wd, *outs, hid, site, ready)


def top(a, dy, wg, wu, wd, first, count, so_far, exchange):
    T, D = a.shape
    FF = wg.shape[-1]
    col = pl.BlockSpec((1, D, C), lambda j: (TOP, 0, first + j))
    act = pl.BlockSpec((T, C), lambda j: (0, first + j))
    W = C * count
    return pl.pallas_call(
        functools.partial(top_body, exchange, count, len(so_far)),
        grid=(count,),
        in_specs=[ANY, ANY, col, col, pl.BlockSpec((1, C, D), lambda j: (TOP, first + j, 0))] + [ANY] * len(so_far) + exchange.in_specs,
        input_output_aliases={5 + i: 3 + i for i in range(len(so_far))},
        out_specs=[UNIT] * 3 + [act, act] + exchange.out_specs,
        out_shape=unit_shapes(count) + [jax.ShapeDtypeStruct((T, FF), BF16)] * 2 + exchange.out_shapes,
        scratch_shapes=[vmem(T, C), vmem(T, D), vmem(T, D), pltpu.SemaphoreType.DMA((2, T // ROWS))] + exchange.scratch,
        compiler_params=exchange.params,
        cost_estimate=pl.CostEstimate(flops=12 * T * D * W, bytes_accessed=20_000_000, transcendentals=T * W),
        name=f"top{first}",
    )(a, dy, wg, wu, wd, *so_far, *exchange.in_arrays)


def bottom_body(exchange, count, *refs):
    own, extra = exchange.split(refs, 5, 3)
    a, dy, gate, up, wd, gg, gu, gd, hid, dgate, dup = own
    site = exchange.sites(extra, count, (5.0, 2.9, 2.9, 2.9))
    for i in range(a.shape[0] // ROWS):
        r = rows_of(i, ROWS)
        dhid = dot(dy[r, :], wd[0], ABT)
        hid[r, :], dgate[r, :], dup[r, :] = swiglu_back(gate[0, r, :], up[0, r, :], dhid)
    site(0)
    put_gradients(a, dy, hid, dgate, dup, gg, gu, gd, site, 1)


def bottom(a, dy, gate, up, wd, first, count, exchange):
    T, D = a.shape
    whole = pl.BlockSpec((T, D), lambda j: (0, 0), pipeline_mode=ONCE)
    act = pl.BlockSpec((1, T, C), lambda j: (first + j, 0, 0))
    W = C * count
    return pl.pallas_call(
        functools.partial(bottom_body, exchange, count),
        grid=(count,),
        in_specs=[whole, whole, act, act, pl.BlockSpec((1, C, D), lambda j: (BOTTOM, first + j, 0))] + exchange.in_specs,
        out_specs=[UNIT] * 3 + exchange.out_specs,
        out_shape=unit_shapes(count) + exchange.out_shapes,
        scratch_shapes=[vmem(T, C)] * 3 + exchange.scratch,
        compiler_params=exchange.params,
        cost_estimate=pl.CostEstimate(flops=8 * T * D * W, bytes_accessed=20_000_000, transcendentals=T * W),
        name=f"bottom{first}",
    )(a, dy, gate, up, wd, *exchange.in_arrays)


def through_body(exchange, steps, *refs):
    own, extra = exchange.split(refs, 6, 1)
    h1, dy, wg, wu, dgate, dup, dh_o, wg_v, wu_v, sem = own
    D = h1.shape[1]
    parts = D // WIDE
    step = pl.program_id(0)
    blocks = [rows_of(k, WIDE) for k in range(parts)]
    loads = [[pltpu.make_async_copy(w.at[TOP, n], v.at[n], sem.at[i, k]) for i, (w, v) in enumerate(((wg, wg_v), (wu, wu_v)))] for k, n in enumerate(blocks)]

    @pl.when(step == 0)
    def _():
        for pair in loads:
            for copy in pair:
                copy.start()

    site = exchange.sites(extra, steps, (2.2,) * (parts - 1) + (3.5,))
    for k, n in enumerate(blocks):
        if k <= 2:

            @pl.when(step == 0)
            def _():
                for pair in loads[k:] if k == 2 else loads[k : k + 1]:
                    for copy in pair:
                        copy.wait()

        dh_o[:, n] = dot(dgate[...], wg_v[n, :], ABT).astype(BF16) + dot(dup[...], wu_v[n, :], ABT).astype(BF16)
        if k < parts - 1:
            site(k)
    by_a = dh_o[...].astype(F32)
    wide = h1[...].astype(F32)
    scale = row_scale(wide)
    by_scale = jnp.sum(by_a * wide, -1, keepdims=True)
    by_mean = by_scale * (-scale * scale * scale / D)
    dh_o[...] = dy[...] + (by_a * scale + wide * by_mean).astype(BF16)
    site(parts - 1)


def through(h1, dy, wg, wu, dgate, dup, exchange):
    T, D = h1.shape
    FF = wg.shape[-1]
    act = pl.BlockSpec((ROWS, FF), lambda j: (j, 0))
    state = pl.BlockSpec((ROWS, D), lambda j: (j, 0))
    return pl.pallas_call(
        functools.partial(through_body, exchange, T // ROWS),
        grid=(T // ROWS,),
        in_specs=[state, state, ANY, ANY, act, act] + exchange.in_specs,
        out_specs=[state] + exchange.out_specs,
        out_shape=[jax.ShapeDtypeStruct((T, D), BF16)] + exchange.out_shapes,
        scratch_shapes=[vmem(D, FF)] * 2 + [pltpu.SemaphoreType.DMA((2, D // WIDE))] + exchange.scratch,
        compiler_params=exchange.params,
        cost_estimate=pl.CostEstimate(flops=4 * T * D * FF, bytes_accessed=60_000_000, transcendentals=T),
        name="through",
    )(h1, dy, wg, wu, dgate, dup, *exchange.in_arrays)


def forward_body(steps, x, dy, wg, wu, wd, gate_o, up_o, a0_o, h1_o, a1_o, gg, gu, gd, dgate_o, dup_o, h, a, acc, hid, sem):
    j = pl.program_id(0)
    T, D = h.shape
    blocks = T // ROWS
    load, load_dy, save_h1, save_a1 = (
        by_rows(*pair, sem.at[i]) if i < 2 else [pltpu.make_async_copy(pair[0].at[r], pair[1].at[r], sem.at[i, k]) for k in range(blocks) for r in (rows_of(k, ROWS),)]
        for i, pair in enumerate(((x, h), (dy, h), (h, h1_o), (a, a1_o)))
    )
    save_a0 = pltpu.make_async_copy(a, a0_o, sem.at[4, 0])

    @pl.when(j == 0)
    def _():
        for copy in load:
            copy.start()
        for i in range(blocks):
            load[i].wait()

            @pl.loop(i * ROWS // LANES, (i + 1) * ROWS // LANES)
            def _(k):
                r = rows_of(k, LANES)
                a[r, :] = normed(h[r, :])
                acc[r, :] = jnp.zeros((LANES, D), F32)

        save_a0.start()

    @pl.when(j < steps)
    def _():
        half = T // 2

        @pl.loop(0, 2)
        def _(i):
            r = rows_of(i, half)
            gate = dot(a[r, :], wg[0])
            up = dot(a[r, :], wu[0])
            gate_o[0, r, :] = gate
            up_o[0, r, :] = up
            hid[r, :] = (gate * lax.logistic(gate) * up).astype(BF16)

        @pl.loop(0, 2)
        def _(i):
            r = rows_of(i, half)
            for k in range(D // WIDE):
                n = span(k, WIDE)
                acc[r, n] += dot(hid[r, :], wd[0, :, n])

    @pl.when(j == steps - 1)
    def _():
        save_a0.wait()
        for i in range(blocks):

            @pl.loop(i * ROWS // LANES, (i + 1) * ROWS // LANES)
            def _(k):
                r = rows_of(k, LANES)
                new = h[r, :] + acc[r, :].astype(BF16)
                h[r, :] = new
                a[r, :] = normed(new)

            save_h1[i].start()
            save_a1[i].start()

    @pl.when(j == steps)
    def _():
        for save, load in zip(save_h1, load_dy, strict=True):
            save.wait()
            load.start()
        top_unit(a, h, wg, wu, wd, gg, gu, gd, dgate_o, dup_o, hid, lambda piece: None, lambda i: load_dy[i].wait())
        for copy in save_a1:
            copy.wait()


def forward(x, dy, wg, wu, wd):
    T, D = x.shape
    FF = wg.shape[-1]
    n = FF // C
    col = pl.BlockSpec((1, D, C), lambda j: (j // n, 0, j % n))
    act = pl.BlockSpec((1, T, C), lambda j: (jnp.minimum(j, n - 1), 0, 0))
    unit = pl.BlockSpec((DEVICES, SHARE, LANES), lambda j: (0, 0, 0), pipeline_mode=ONCE)
    back = pl.BlockSpec((T, C), lambda j: (0, 0), pipeline_mode=ONCE)
    return pl.pallas_call(
        functools.partial(forward_body, n),
        grid=(n + 1,),
        in_specs=[ANY, ANY, col, col, pl.BlockSpec((1, C, D), lambda j: (j // n, j % n, 0))],
        out_specs=[act, act, ANY, ANY, ANY, unit, unit, unit, back, back],
        out_shape=[jax.ShapeDtypeStruct((n, T, C), F32)] * 2
        + [jax.ShapeDtypeStruct((T, D), BF16)] * 3
        + unit_shapes(1)
        + [jax.ShapeDtypeStruct((T, FF), BF16)] * 2,
        scratch_shapes=[vmem(T, D), vmem(T, D), vmem(T, D, dtype=F32), vmem(T, C), pltpu.SemaphoreType.DMA((5, T // ROWS))],
        compiler_params=pltpu.CompilerParams(vmem_limit_bytes=VMEM),
        cost_estimate=pl.CostEstimate(flops=6 * T * D * FF, bytes_accessed=100_000_000, transcendentals=T * FF),
        name="forward",
    )(x, dy, wg, wu, wd)


def new_values(w, m, v, g):
    m = 0.9 * m + 0.1 * g
    v = 0.95 * v + 0.05 * g * g
    step = m * lax.rsqrt(v + 1e-8) + 0.1 * w
    return (w - 0.02 * step).astype(BF16), m, v


def adamw_body(*refs):
    g, w, m, v = (refs[span(i, 3)] for i in range(4))
    new = refs[-9:]
    for which in MATRICES:

        def take(rows, cols, grad):
            at = (0, rows, cols)
            done = new_values(w[which][at].astype(F32), m[which][at], v[which][at], grad.astype(F32))
            for out, value in zip(new[which::3], done, strict=True):
                out[at] = value

        _, rows, cols = w[which].shape
        if which < 2:
            for i in range(rows // SHARE):
                for j in range(SIDE):
                    take(rows_of(i, SHARE), rows_of(j, LANES), g[which][i * SIDE + j, 0])
        else:
            for i in range(rows // TILE):
                for j in range(cols // LANES):
                    half, tile = divmod(j, SHARE // TILE)
                    take(rows_of(i, TILE), rows_of(j, LANES), g[which][2 * i + half, 0, rows_of(tile, TILE), :])


def adamw(summed, arrays, layer, first, count, so_far):
    D = arrays[0].shape[1]
    summed = summed.reshape(DEVICES, 3, SHARE * count, LANES)

    def grad(which):
        return pl.BlockSpec((DEVICES // STEPS, 1, SHARE, LANES), lambda i: (i % STEPS, which, i // STEPS, 0))

    wide = pl.BlockSpec((1, D // STEPS, C), lambda i: (layer, i % STEPS, first + i // STEPS))
    tall = pl.BlockSpec((1, C // STEPS, D), lambda i: (layer, first * STEPS + i, 0))
    nine = [wide, wide, tall] * 3
    return pl.pallas_call(
        adamw_body,
        grid=(count * STEPS,),
        in_specs=[grad(which) for which in MATRICES] + nine + [ANY] * len(so_far),
        out_specs=nine,
        out_shape=[jax.ShapeDtypeStruct(a.shape, a.dtype) for a in arrays],
        input_output_aliases={12 + i: i for i in range(len(so_far))},
        compiler_params=pltpu.CompilerParams(vmem_limit_bytes=VMEM),
        cost_estimate=pl.CostEstimate(flops=1_000_000_000 * count, bytes_accessed=66 * D * C * count, transcendentals=3 * D * C * count),
        name=f"adamw{layer}_{first}",
    )(summed, summed, summed, *arrays, *so_far)


def solution(mesh):
    def step(x, dy, *arrays):
        x, dy = x[0], dy[0]
        weights = arrays[:3]
        *gates, wd = weights
        one, three, four = (SHARE * count for count in (1, 3, 4))
        gate0, up0, a0, h1, a1, *out = forward(x, dy, *weights)
        g0, back = out[:3], out[3:]
        *out, s0 = top(a1, dy, *weights, 1, 3, back, Exchange(1, (Scatter(one), g0)))
        g1, back = out[:3], out[3:]
        *out, s1 = top(a1, dy, *weights, 4, 3, back, Exchange(2, (Scatter(three), g1)))
        g2, back = out[:3], out[3:]
        dh1, s2 = through(h1, dy, *gates, *back, Exchange(3, (Scatter(three), g2)))
        g3 = bottom(a0, dh1, gate0, up0, wd, 0, 3, Exchange())
        *g4, s3 = bottom(a0, dh1, gate0, up0, wd, 3, 4, Exchange(4, (Scatter(three), g3)))
        (s4,) = Exchange(5, (Scatter(four), g4)).alone()
        parts = [jnp.concatenate([s0, s1, s2], 1), s3, s4]
        summed = [lax.all_gather(part, "dp", axis=0, tiled=False) for part in parts]
        new = ()
        for g, layer, first, count in zip(summed, (TOP, BOTTOM, BOTTOM), (0, 0, 3), (7, 3, 4), strict=True):
            new = adamw(g, arrays, layer, first, count, new)
        return tuple(new)

    whole = P(None, None, None)
    return jax.shard_map(
        step, mesh=mesh, in_specs=(P(("rep", "dp"), None, None),) * 2 + (whole,) * 9, out_specs=(P("rep", None, None),) * 9, check_vma=False
    )
```
